32 devices in a mesh: dp: 4 (over z), tp: 8 (over y, x, core).
Axes of the slice: x: 2, y: 2, z: 4, core: 2. Of those that a mesh axis runs over, the one named last changes fastest.
Arguments:
- hidden: bfloat16 [16, 1024, 1024], P('dp')
- labels: int32 [16, 1024], P('dp')
- loss_mask: int32 [16, 1024], P('dp')
- norm_gain: bfloat16 [1024], replicated
- w_out: bfloat16 [1024, 50304], P(None, 'tp')
Outputs:
- output 1: float32 [], replicated
- output 2: bfloat16 [16, 1024, 1024], P('dp')
- output 3: float32 [1024], replicated
- output 4: float32 [1024, 50304], P(None, 'tp')
All inputs are finite; a program needn't handle non-finite values.
Results may differ from the reference program's by a relative error of at most 0.001.
Values sent between devices are 32-bit elements.
A program may use at most 1 GiB of HBM per device.

```python
import jax
import jax.numpy as jnp
from jax import lax

D_MODEL = 1024
VOCAB = 50304
BATCH = 16
SEQ = 1024
EPS_NORM = 1e-5


def draw_mask(key_shift, key_draw):
    row_ids = jnp.arange(BATCH, dtype=jnp.int32)[:, None]
    shift_rows = jax.random.randint(key_shift, (), 0, BATCH, jnp.int32)
    keep_pct = 30 + (70 * ((row_ids + shift_rows) % BATCH)) // max(BATCH - 1, 1)
    draw_vals = jax.random.randint(key_draw, (BATCH, SEQ), 0, 100, jnp.int32)
    first_pos = jnp.arange(SEQ, dtype=jnp.int32)[None, :] == 0
    return jnp.where(first_pos | (draw_vals < keep_pct), 1, 0).astype(jnp.int32)


def setup_inputs(seed: int = 0) -> dict:
    root_key = jax.random.key(seed)
    sub_keys = jax.random.split(root_key, 6)
    hidden = jax.random.normal(sub_keys[0], (BATCH, SEQ, D_MODEL), jnp.float32).astype(jnp.bfloat16)
    labels = jax.random.randint(sub_keys[1], (BATCH, SEQ), 0, VOCAB, jnp.int32)
    loss_mask = draw_mask(sub_keys[2], sub_keys[3])
    norm_gain = (1.0 + 0.3 * jax.random.normal(sub_keys[4], (D_MODEL,), jnp.float32)).astype(jnp.bfloat16)
    w_scale = 2.0 * D_MODEL ** -0.5
    w_out = (jax.random.normal(sub_keys[5], (D_MODEL, VOCAB), jnp.float32) * w_scale).astype(jnp.bfloat16)
    return {"hidden": hidden, "labels": labels, "loss_mask": loss_mask, "norm_gain": norm_gain, "w_out": w_out}


def reference(hidden, labels, loss_mask, norm_gain, w_out):
    gain_f = norm_gain.astype(jnp.float32)
    mask_f = loss_mask.astype(jnp.float32)
    mask_count = jnp.sum(mask_f)
    vocab_ids = jnp.arange(VOCAB, dtype=jnp.int32)[None, :]

    def row_step(state_in, row_data):
        loss_acc, gain_acc, weight_acc = state_in
        h_row, label_row, mask_row = row_data
        x_row = h_row.astype(jnp.float32)
        inv_rms = lax.rsqrt(jnp.mean(x_row * x_row, axis=-1, keepdims=True) + EPS_NORM)
        x_hat = x_row * inv_rms
        u_row = (x_hat * gain_f).astype(jnp.bfloat16)
        logits = jnp.dot(u_row, w_out, preferred_element_type=jnp.float32)
        row_max = jnp.max(logits, axis=-1, keepdims=True)
        log_norm = row_max + jnp.log(jnp.sum(jnp.exp(logits - row_max), axis=-1, keepdims=True))
        is_label = vocab_ids == label_row[:, None]
        target = jnp.sum(jnp.where(is_label, logits, 0.0), axis=-1, keepdims=True)
        loss_acc = loss_acc + jnp.sum(mask_row[:, None] * (log_norm - target))
        prob_row = jnp.exp(logits - log_norm)
        d_logits = (jnp.where(is_label, prob_row - 1.0, prob_row) * (mask_row / mask_count)[:, None]).astype(jnp.bfloat16)
        du_row = lax.dot_general(d_logits, w_out, (((1,), (1,)), ((), ())), preferred_element_type=jnp.float32)
        weight_acc = weight_acc + lax.dot_general(u_row, d_logits, (((0,), (0,)), ((), ())), preferred_element_type=jnp.float32)
        gain_acc = gain_acc + jnp.sum(du_row * x_hat, axis=0)
        d_xhat = du_row * gain_f
        dx_row = inv_rms * (d_xhat - x_hat * jnp.mean(d_xhat * x_hat, axis=-1, keepdims=True))
        return (loss_acc, gain_acc, weight_acc), dx_row.astype(jnp.bfloat16)

    init_state = (jnp.zeros((), jnp.float32), jnp.zeros((D_MODEL,), jnp.float32), jnp.zeros((D_MODEL, VOCAB), jnp.float32))
    final_state, d_hidden = lax.scan(row_step, init_state, (hidden, labels, mask_f))
    loss_sum, d_gain, d_w_out = final_state
    return (loss_sum / mask_count, d_hidden, d_gain, d_w_out)
```

```python
import functools

import jax
import jax.numpy as jnp
from jax import lax
from jax.experimental import pallas as pl
from jax.experimental.pallas import tpu as pltpu
from jax.sharding import PartitionSpec as P

EPS_NORM = 1e-5
LOG2E = 1.4426950408889634
F32 = jnp.float32
BF16 = jnp.bfloat16
ANY = pl.ANY
NT = (((1,), (1,)), ((), ()))
TN = (((0,), (0,)), ((), ()))


class Sizes:
    def __init__(self, tokens, width, vocab, pv, own, oc, osub, ac, asub, st):
        self.T, self.D, self.V = tokens, width, vocab
        self.PV, self.ST = pv, st
        self.OW, self.OC, self.OS = own, oc, osub
        self.RA, self.AC, self.AS = vocab - 2 * own, ac, asub
        self.PT = tokens // 4
        self.SL = tokens // 8
        self.SK = self.SL // 2
        self.NPV = vocab // pv
        self.RV = vocab - self.NPV * pv
        self.SG = tokens // 32
        self.AG = (asub + 15) // 16 * 8
        self.NOS, self.NAS = own // osub, self.RA // asub


def _kernel(z_, h, lab, msk, gain, wT, dw, dh, dg, loss, zh, unf, rb, rc, dub0, dub1, dub2,
            uv, unv, pb, zr, wr, da, da2, stg, hst, dhs, m8, s8, t8, lab8, lsev, mnv, mskn, labn, sts, strv, cntb, cntr, lsb, lsr, dgb, dgr,
            zi, wi, zo, hs, lg, a1_s, a1_r, a2_s, a2_r, a3_s, a3_r, h1_s, h1_r, h2_s, h2_r, h3_s, h3_r, lo, la, ag_s, ag_r, du_s, du_r, dl, ct_s, ct_r, st_s, st_r, me_s, me_r, ls_s, ls_r, dg_s, dg_r):
    T, D, V = z_.T, z_.D, z_.V
    PV, ST, PT, SL, SK, NPV, RV, SG = z_.PV, z_.ST, z_.PT, z_.SL, z_.SK, z_.NPV, z_.RV, z_.SG
    OW, OC, OS, RA, AC, AS, AG, NOS, NAS = z_.OW, z_.OC, z_.OS, z_.RA, z_.AC, z_.AS, z_.AG, z_.NOS, z_.NAS
    NS = PT // ST
    d, t = lax.axis_index("dp"), lax.axis_index("tp")
    core, xx, yy = t % 2, (t // 2) % 2, t // 4
    tc, tx, ty = t + 1 - 2 * core, t + 2 - 4 * xx, t + 4 - 8 * yy
    da_, db_ = d + 1 - 2 * (d % 2), 3 - d
    df_ = 3 - da_
    mid = ((d + 1) // 2) % 2 == 1
    end = ((d + 1) // 2) % 2 == 0
    pc, px, py, pa, pbq, pf_ = (d, tc), (d, tx), (d, ty), (da_, t), (db_, t), (df_, t)
    own0 = (d // 3) * OW
    near0 = (da_ // 3) * OW
    far0 = OW - near0

    pair, quad = range(2), range(4)

    def al(x, m):
        return x if isinstance(x, int) else pl.multiple_of(x, m)

    def a8(x):
        return al(x, 8)

    def a16(x):
        return al(x, 16)

    def tof(x):
        return float(x) if isinstance(x, int) else x.astype(F32)

    def rcopy(src, dst, ssem, rsem, dev):
        return pltpu.make_async_remote_copy(src_ref=src, dst_ref=dst, send_sem=ssem, recv_sem=rsem, device_id=dev, device_id_type=pl.DeviceIdType.MESH)

    cp = pltpu.make_async_copy

    bar = pltpu.get_barrier_semaphore()
    for dev in (pc, px, py, pa, pbq, pf_):
        pl.semaphore_signal(bar, inc=1, device_id=dev, device_id_type=pl.DeviceIdType.MESH)
    hsl = cp(h.at[pl.ds(a16(t * SL), SL), :], wr.at[2, :SL, :], hs.at[4])
    hsl.start()

    def hcopy(b):
        return cp(h.at[pl.ds(a16(b * PT), PT), :], unv.at[pl.ds(a16(b * PT), PT), :], hs.at[b])

    for b in quad:
        hcopy(b).start()

    def wcopy(r0, n, slot):
        return cp(wT.at[pl.ds(r0, n), :], wr.at[slot, :n, :], wi.at[slot])

    wcopy(0, PV, 0).start()
    hsl.wait()

    def rms(hb):
        x = hb.astype(F32)
        inv = lax.rsqrt(jnp.mean(x * x, axis=1, keepdims=True) + EPS_NORM)
        return x * inv, inv

    xh, _ = rms(wr[2, :SL, :])
    ub0 = RA + OW - SL
    pb[ub0:ub0 + SL, :] = (xh * gain[...]).astype(BF16).astype(F32)
    sub_iota = lax.broadcasted_iota(jnp.int32, (8, T), 0).astype(F32)
    toff = (t * V).astype(F32)
    lab8[0] = jnp.broadcast_to(lab[...] - toff, (8, T)) - sub_iota
    cntb[0] = jnp.broadcast_to(jnp.sum(msk[...], axis=1, keepdims=True), (8, 128))
    m8[...] = jnp.full((8, T), -jnp.inf, F32)
    s8[...] = jnp.zeros((8, T), F32)
    t8[...] = jnp.zeros((8, T), F32)
    pl.semaphore_wait(bar, 6)

    def urow(tt, u):
        return unf.at[u // 2, pl.ds(a8(tt * SL + (u % 2) * SK), SK), :]

    def zsend(u, dev):
        return rcopy(pb.at[pl.ds(ub0 + (u % 2) * SK, SK), :], urow(t, u), ag_s.at[u, 0], ag_r.at[u, 0], dev)

    def metas(slot, dev):
        return [rcopy(src, dst.at[slot + o], me_s.at[i, slot], me_r.at[i, slot], dev)
                for i, (src, dst, o) in enumerate(((lab, labn, 0), (msk, mskn, 0), (lsev.at[0], lsev, 1)))]

    def ag(u, j):
        tf, tg = (tx, ty) if u % 2 == 0 else (ty, tx)
        pf, pg = (px, py) if u % 2 == 0 else (py, px)
        tfg = tf + tg - t
        who, dev = ((None, None), (t, pf), (t, pg), (tf, pg), (t, pc), (tf, pc), (tg, pc), (tfg, pc))[j]
        return rcopy(urow(who, u), urow(who, u), ag_s.at[u, j], ag_r.at[u, j], dev)

    def cnt2(i):
        return rcopy(cntb.at[i], cntr.at[i], ct_s.at[i], ct_r.at[i], (pa, pbq)[i])

    def lss2(i):
        return rcopy(lsb.at[i], lsr.at[i], ls_s.at[i], ls_r.at[i], (pa, pbq)[i])

    cnt2(0).start()

    @pl.when(mid)
    def _():
        for c in metas(1, pa)[:2] + metas(2, pf_)[:2]:
            c.start()

    @pl.when(end)
    def _():
        for c in metas(0, pbq)[:2]:
            c.start()
        for u in pair:
            zsend(u, pbq).start()

    def e1(u):
        zsend(u, pa).wait_recv()
        for j in (1, 2, 4):
            ag(u, j).start()

    def e23(u):
        ag(u, 1).wait_recv()
        ag(u, 3).start()
        ag(u, 5).start()
        ag(u, 2).wait_recv()
        ag(u, 6).start()

    def e4(u):
        ag(u, 3).wait_recv()
        ag(u, 7).start()

    def ec(_):
        cnt2(0).wait()
        cntb[1] = cntb[0] + cntr[0]
        cnt2(1).start()

    def near(_):
        for u in range(2, 4):
            zsend(u, pa).start()

    def far(_):
        for u in range(4, 6):
            zsend(u, pf_).start()

    def run(evs, names):
        for i in range(0, len(evs), 2):
            names[evs[i]](int(evs[i + 1]))

    enames = dict(i=e1, j=e23, k=e4)
    early = dict(d="i0", g="i1", h="j0")

    def stats(z, n, base, cols):
        labb = lab8[0, :, cols] - tof(base)
        m, s, tg = m8[:, cols], s8[:, cols], t8[:, cols]
        for w0 in range(0, n, 128):
            kk = min(128, n - w0)
            z3 = z[w0:w0 + kk].reshape(kk // 8, 8, ST)
            mn = jnp.maximum(m, jnp.max(z3, axis=0))
            mc = mn * LOG2E
            s = s * jnp.exp2(m * LOG2E - mc) + jnp.sum(jnp.exp2(z3 * LOG2E - mc[None]), axis=0)
            for i in range(kk // 8):
                tg = tg + jnp.where(labb == float(w0 + 8 * i), z3[i], 0.0)
            m = mn
        m8[:, cols], s8[:, cols], t8[:, cols] = m, s, tg

    def zout(tb, r0, n):
        return cp(zr.at[tb, :n, :], zh.at[tb, pl.ds(r0, n), :], zo.at[tb])

    def fwd_pieces(ws, tbs, r0, n):
        for tb in tbs:
            for k in range(NS):
                cols = pl.ds(al(tb * PT + k * ST, ST), ST)
                z = lax.dot_general(wr[ws, :n, :], uv[cols, :], NT, preferred_element_type=F32)
                zr[tb, :n, pl.ds(k * ST, ST)] = z
                stats(z, n, r0, cols)
            zout(tb, r0, n).start()

    @pl.loop(0, NPV * 2)
    def _(q):
        v, half = q // 2, q % 2
        r0 = a16(v * PV)
        ws = v % 2

        @pl.when(half == 0)
        def _():
            wcopy(r0, PV, ws).wait()

            @pl.when(v + 1 < NPV)
            def _():
                wcopy(a16(r0 + PV), PV, 1 - ws).start()

        @pl.when(v == 0)
        def _():
            for k in pair:
                tb = 2 * half + k
                hcopy(tb).wait()
                rows = pl.ds(a16(tb * PT), PT)
                xb, _ = rms(unv[rows, :])
                uv[rows, :] = (xb * gain[...]).astype(BF16)

        @pl.when(v > 0)
        def _():
            for k in pair:
                zout(2 * half + k, 0, PV).wait()

        fwd_pieces(ws, (2 * half, 2 * half + 1), r0, PV)

        def at(i):
            return (half == 1) & (v == min(i, NPV - 1))

        @pl.when(at(1))
        def _():
            ec(0)

        @pl.when(mid & at(6))
        def _():
            near(0)

        for ch, evs in early.items():
            @pl.when(end & at(ord(ch) - ord("a")))
            def _():
                run(evs, enames)

    wcopy(NPV * PV, RV, 2).start()
    wcopy(NPV * PV, RV, 2).wait()

    @pl.loop(0, 4)
    def _(tb):
        zout(tb, 0, PV).wait()
        fwd_pieces(2, (tb,), NPV * PV, RV)

    m = jnp.max(m8[...], axis=0, keepdims=True)
    s = jnp.sum(s8[...] * jnp.exp(m8[...] - m), axis=0, keepdims=True)
    sts[0, 0:1, :] = m + jnp.log(s)
    sts[0, 1:2, :] = jnp.sum(t8[...], axis=0, keepdims=True)
    for r, dev in enumerate((pc, px, py)):
        c = rcopy(sts.at[r], strv.at[r], st_s.at[r], st_r.at[r], dev)
        c.start()
        c.wait()
        a, b = sts[r, 0:1, :], strv[r, 0:1, :]
        hi = jnp.maximum(a, b)
        sts[r + 1, 0:1, :] = hi + jnp.log(jnp.exp(a - hi) + jnp.exp(b - hi))
        sts[r + 1, 1:2, :] = sts[r, 1:2, :] + strv[r, 1:2, :]
    lse, tgt = sts[3, 0:1, :], sts[3, 1:2, :]
    lsev[0] = lse * LOG2E
    cnt2(1).wait()
    cnt = (cntb[1] + cntr[1])[0:1, 0:1]
    mnv[0] = msk[...] / cnt
    lsb[0] = jnp.broadcast_to(jnp.sum(msk[...] * (lse - tgt), axis=1, keepdims=True), (8, 128))

    @pl.when(mid)
    def _():
        metas(1, pa)[2].start()
        metas(2, pf_)[2].start()
        far(0)

    @pl.when(end)
    def _():
        metas(0, pbq)[2].start()
        run("i2j1k0", enames)

    lss2(0).start()
    for tb in quad:
        zout(tb, 0, RV).wait()

    def gmat(z, who, base, cols):
        one = 0 if who is None else 1
        labb = lab8[one, :, cols] - tof(base)
        lse2 = lsev[0 if who is None else who + 1, :, cols]
        mn = jnp.broadcast_to(mnv[one, :, cols], (8, ST))
        p = jnp.exp2(z * LOG2E - lse2)
        rows = []
        for i in range(z.shape[0] // 8):
            pi = p[8 * i:8 * i + 8]
            rows.append(jnp.where(labb == float(8 * i), pi - 1.0, pi) * mn)
        return jnp.concatenate(rows, axis=0).astype(BF16)

    def arow(i):
        return pl.ds(a8(i * AS), AS)

    def awr(i):
        return dw.at[pl.ds(a8(2 * OW + i * AS), AS), :]

    def a1(i):
        return rcopy(pb.at[arow(i), :], rb.at[arow(i), :], a1_s.at[i], a1_r.at[i], pa)

    def a2(i):
        return rcopy(pb.at[arow(i), :], rc.at[arow(i), :], a2_s.at[i], a2_r.at[i], pbq)

    def a3(i):
        return rcopy(pb.at[arow(i), :], awr(i), a3_s.at[i], a3_r.at[i], pa)

    def alocal(i):
        return cp(pb.at[arow(i), :], awr(i), la.at[i])

    def grab(src, i):
        for o in range(0, AS, AG):
            n = min(AG, AS - o)
            rows = pl.ds(a8(i * AS + o), n)
            c = cp(src.at[rows, :], stg.at[:n, :], lg.at[0])
            c.start()
            c.wait()
            pb[rows, :] = pb[rows, :] + stg[:n, :]

    def ev_a1(i):
        a1(i).wait_recv()
        grab(rb, i)
        a2(i).start()

    def ev_a2(i):
        a2(i).wait()
        grab(rc, i)
        alocal(i).start()
        a3(i).start()

    def drow(base, i):
        return dw.at[pl.ds(a8(base + i * OS), OS), :]

    def prow(i):
        return pb.at[pl.ds(a8(RA + i * OS), OS), :]

    def h1(i):
        return rcopy(prow(i), drow(own0, i), h1_s.at[i], h1_r.at[i], pa)

    def h2(i):
        return rcopy(drow(near0, i), drow(near0, i), h2_s.at[i], h2_r.at[i], pbq)

    def h3(i):
        return rcopy(drow(far0, i), drow(far0, i), h3_s.at[i], h3_r.at[i], pa)

    def hop(i):
        h1(i).wait_recv()
        h2(i).start()
        if not isinstance(i, int) or i > 0:
            h2(i - 1).wait_recv()
            h3(i - 1).start()

    def hlocal(i):
        return cp(prow(i), drow(own0, i), lo.at[i])

    H = SG // 2
    k0 = core * (4 * SG)

    def lev(k):
        fb, sb = (xx, yy) if k == 0 else (yy, xx)
        pf, ps = (px, py) if k == 0 else (py, px)
        k1 = k * 2 * SG + fb * SG
        return pf, ps, k1, k * 2 * SG + (1 - fb) * SG, k1 + sb * H, k1 + (1 - sb) * H

    def ducopy(g, j, k=0):
        pf, ps, k1, o1, k2, o2 = lev(k)
        b = g % 2
        base = g * PT + k0
        sems = (du_s.at[g, j, k], du_r.at[g, j, k])
        if j == 0:
            return rcopy(da.at[b, pl.ds(a8(4 * SG - k0), 4 * SG), :], dub0.at[g], *sems, pc)
        if j == 1:
            return rcopy(da2.at[b, pl.ds(a8(o1), SG), :], dub1.at[g, k], *sems, pf)
        if j == 2:
            return rcopy(da2.at[b, pl.ds(a8(o2), H), :], dub2.at[g, k], *sems, ps)
        if j == 3:
            return rcopy(dhs.at[b, k], dh.at[pl.ds(a8(base + k2), H), :], *sems, ps)
        r, n, dev = ((k1, SG, pf), (0, 4 * SG, pc))[j - 4]
        r = dh.at[pl.ds(a8(base + r), n), :]
        return rcopy(r, r, *sems, dev)

    def add_in(buf, g, src, k, k2, n):
        @pl.loop(0, n // SG)
        def _(i):
            c = cp(buf.at[pl.ds(a8(i * SG), SG), :], stg.at[:SG, :], lg.at[1])
            c.start()
            c.wait()
            da2[g % 2, pl.ds(a8(k2 + i * SG), SG), :] = src[g % 2, pl.ds(a8(k + i * SG), SG), :] + stg[:SG, :]

    def d2(g):
        ducopy(g, 0).wait_recv()
        for k in pair:
            if g >= 2:
                ducopy(g - 2, 1, k).wait_send()
                ducopy(g - 2, 2, k).wait_send()
        add_in(dub0.at[g], g, da, k0, 0, 4 * SG)
        for k in pair:
            ducopy(g, 1, k).start()

    def d3(g):
        for k in pair:
            ducopy(g, 1, k).wait_recv()
            add_in(dub1.at[g, k], g, da2, lev(k)[2], lev(k)[2], SG)
            ducopy(g, 2, k).start()

    def dhlocal(g, k):
        return cp(dhs.at[g % 2, k], dh.at[pl.ds(a8(g * PT + k0 + lev(k)[4]), H), :], dl.at[g, k])

    def d4(g):
        for k in pair:
            k2 = lev(k)[4]
            ch = cp(h.at[pl.ds(a8(g * PT + k0 + k2), H), :], hst, lg.at[2])
            ch.start()
            ducopy(g, 2, k).wait_recv()
            c = cp(dub2.at[g, k], stg.at[:H, :], lg.at[1])
            c.start()
            c.wait()
            if g >= 2:
                ducopy(g - 2, 3, k).wait_send()
            ch.wait()
            xb, inv = rms(hst[...])
            du = da2[g % 2, pl.ds(a8(k2), H), :] + stg[:H, :]
            part = jnp.sum((du * xb).reshape(H // 8, 8, D), axis=0)
            dgb[0] = part if g == 0 and k == 0 else dgb[0] + part
            a = du * gain[...]
            dhs[g % 2, k] = inv * (a - xb * jnp.mean(a * xb, axis=1, keepdims=True))
            dhlocal(g, k).start()
            ducopy(g, 3, k).start()

    def d5(g):
        for k in pair:
            ducopy(g, 3, k).wait_recv()
            dhlocal(g, k).wait()
            ducopy(g, 4, k).start()

    def d6(g):
        for k in pair:
            ducopy(g, 4, k).wait_recv()
        ducopy(g, 5).start()

    dgdev = (pc, px, py, pa, pbq)

    def dgc(r):
        return rcopy(dgb.at[r], dgr.at[r], dg_s.at[r], dg_r.at[r], dgdev[r])

    def ev_dg(r):
        if r > 0:
            dgc(r - 1).wait()
            dgb[r] = dgb[r - 1] + dgr[r - 1]
        if r < 5:
            dgc(r).start()

    def ev_ls():
        lss2(0).wait()
        lsb[1] = lsb[0] + lsr[0]
        lss2(1).start()

    dnames = dict(a=d2, b=d3, c=d4, d=d5, e=d6, g=ev_dg)
    mnames = dict(p=ev_a1, q=ev_a2, h=hop)
    duev = dict(m1="a0", m2="b0a1", m3="c0a2", f3="b1")
    muev = dict(m1="p0", f1="p1", m2="q0p2", f2="q1", m3="p3q2")

    def poll(kind, idx):
        for i in quad:
            key = kind + str(i)
            if key in duev:
                @pl.when(idx == i)
                def _():
                    run(duev[key], dnames)
            if key in muev:
                @pl.when((idx == i) & mid)
                def _():
                    run(muev[key], mnames)

    def zin(tb, r0, n, slot):
        return cp(zh.at[tb, pl.ds(r0, n), :], zr.at[slot, :n, :], zi.at[slot])

    def uin(sh, b):
        n = PT // 2
        return cp(unf.at[sh, pl.ds(a8(b * n), n), :], zr.at[b % 4, :n, :], zi.at[b % 4])

    def convert(sh):
        for k in pair:
            for j in range(4, 8):
                ag_wait = rcopy(unf.at[0, :SK, :], unf.at[0, :SK, :], ag_s.at[2 * sh + k, j], ag_r.at[2 * sh + k, j], pc)
                ag_wait.wait_recv()
        for i, dst in enumerate((labn, mskn, lsev)):
            rcopy(dst.at[0], dst.at[0], me_s.at[i, sh], me_r.at[i, sh], pa).wait_recv()
        mnv[1] = mskn[sh] / cnt
        lab8[1] = jnp.broadcast_to(labn[sh] - toff, (8, T)) - sub_iota
        for b in quad:
            uin(sh, b).start()

    def own_start(g0, n):
        for tb in quad:
            zin(tb, g0, n, tb).start()

    def chunk_own(r0, g0, n, more):
        rows = pl.ds(r0, n)
        pb[rows, :] = jnp.zeros((n, D), F32)

        @pl.loop(0, 4)
        def _(tb):
            zin(tb, g0, n, tb).wait()
            gs = []
            for k in range(NS):
                gs.append(gmat(zr[tb, :n, pl.ds(k * ST, ST)], None, g0, pl.ds(al(tb * PT + k * ST, ST), ST)))
            g = jnp.concatenate(gs, axis=1)

            @pl.when(more)
            def _():
                zin(tb, a8(g0 + n), n, tb).start()

            pb[rows, :] += jnp.dot(g, uv[pl.ds(a16(tb * PT), PT), :], preferred_element_type=F32)

    def chunk_far(r0, g0, n, sh, first):
        wcopy(g0, n, 0).start()
        wcopy(g0, n, 0).wait()
        rows = pl.ds(r0, n)

        @pl.loop(0, 2)
        def _(q):
            @pl.when(first)
            def _():
                for b in quad:
                    uin(sh, 4 * q + b).wait()
                    unv[pl.ds(a16((4 * q + b) * (PT // 2)), PT // 2), :] = zr[b, :PT // 2, :].astype(BF16)

                @pl.when(q == 0)
                def _():
                    for b in range(4, 8):
                        uin(sh, b).start()

            for j in pair:
                gs = []
                for k in range(NS):
                    cols = pl.ds(al((2 * q + j) * PT + k * ST, ST), ST)
                    z = lax.dot_general(wr[0, :n, :], unv[cols, :], NT, preferred_element_type=F32)
                    gs.append(gmat(z, sh, g0, cols))
                g = jnp.concatenate(gs, axis=1)
                pb[rows, :] += jnp.dot(g, unv[pl.ds(a16((2 * q + j) * PT), PT), :], preferred_element_type=F32)

    def du_piece(b, tb, v, r0, n):
        for k in range(NS):
            g = gmat(zr[v % 4, :n, pl.ds(k * ST, ST)], None, r0, pl.ds(al(tb * PT + k * ST, ST), ST))
            da[b, pl.ds(k * ST, ST), :] += lax.dot_general(g, wr[v % 3, :n, :], TN, preferred_element_type=F32)

    def du_block(tb):
        b = tb % 2

        def pz(v, n):
            return zin(tb, a16(v * PV), n, v % 4)

        def pw(v, n):
            return wcopy(a16(v * PV), n, v % 3)

        for g in range(2, 4):
            @pl.when(tb == g)
            def _():
                ducopy(g - 2, 0).wait_send()

        for v in pair:
            pz(v, PV).start()
            pw(v, PV).start()
        pz(2, PV).start()
        da[b] = jnp.zeros((PT, D), F32)

        @pl.loop(0, NPV)
        def _(v):
            pz(v, PV).wait()
            pw(v, PV).wait()
            for o, f in ((3, pz), (2, pw)):
                @pl.when(v + o < NPV)
                def _():
                    f(v + o, PV).start()

                @pl.when(v + o == NPV)
                def _():
                    f(NPV, RV).start()

            du_piece(b, tb, v, v * PV, PV)

            @pl.when(v == NPV // 2)
            def _():
                poll("m", tb)

        pz(NPV, RV).wait()
        pw(NPV, RV).wait()
        du_piece(b, tb, NPV, NPV * PV, RV)
        poll("f", tb)
        for g in quad:
            @pl.when(tb == g)
            def _():
                ducopy(g, 0).start()

    shev = dict(s00="j3i5", s01="k2", s03="j4", s04="k3", s11="j5", s12="k4", s14="k5")

    own_start(2 * OW, AC)

    @pl.loop(0, RA // AC)
    def _(c):
        chunk_own(a8(c * AC), a8(2 * OW + c * AC), AC, c + 1 < RA // AC)

        for i, evs in enumerate(("", "", "i3j2")):
            if evs:
                @pl.when(end & (c == i))
                def _():
                    run(evs, enames)

        @pl.when(end)
        def _():
            for s in range(AC // AS):
                a1(c * (AC // AS) + s).start()

    @pl.when(end)
    def _():
        own_start(a8(own0), OC)

        @pl.loop(0, OW // OC)
        def _(c):
            @pl.when(c == (ub0 - RA) // OC)
            def _():
                for u in pair:
                    zsend(u, pbq).wait_send()

            chunk_own(a8(RA + c * OC), a8(own0 + c * OC), OC, c + 1 < OW // OC)
            for i, evs in enumerate(("", "", "k1i4", "", "")):
                if evs:
                    @pl.when(c == i)
                    def _():
                        run(evs, enames)

        @pl.loop(0, 3)
        def _(sh):
            convert(sh)

            @pl.loop(0, OW // OC)
            def _(c):
                chunk_far(a8(RA + c * OC), a8(own0 + c * OC), OC, sh, c == 0)
                for x, evs in shev.items():
                    @pl.when((sh == int(x[1])) & (c == int(x[2])))
                    def _():
                        run(evs, enames)

                @pl.when(sh == 2)
                def _():
                    for s in range(OC // OS):
                        i = c * (OC // OS) + s
                        hlocal(i).start()
                        h1(i).start()

    @pl.loop(0, 4)
    def _(tb):
        du_block(tb)

    @pl.when(mid)
    def _():
        run("p4q3c1a3b2d0p5q4c2b3d1e0q5c3g0d2g1e1h0g2d3e2h1e3h2", {**dnames, **mnames})

        @pl.loop(3, NOS)
        def _(i):
            hop(i)

        h2(NOS - 1).wait_recv()
        h3(NOS - 1).start()

    @pl.when(end)
    def _():
        run("c1a3b2d0c2b3d1e0c3g0d2g1e1g2d3e2e3", dnames)

    run("g3g4", dnames)
    ev_ls()
    run("g5", dnames)

    dg[...] = jnp.sum(dgb[5], axis=0, keepdims=True)
    lss2(1).wait()
    loss[...] = (lsb[1] + lsr[1]) / cnt
    for g in quad:
        ducopy(g, 5).wait()
        for k in pair:
            ducopy(g, 4, k).wait_send()
            if g >= 2:
                for j in (1, 2, 3):
                    ducopy(g, j, k).wait_send()
        if g >= 2:
            ducopy(g, 0).wait_send()

    @pl.when(mid)
    def _():
        for u in range(2, 6):
            zsend(u, pa).wait_send()
        for c in metas(1, pa) + metas(2, pf_):
            c.wait_send()

        @pl.loop(0, NAS)
        def _(i):
            a3(i).wait_send()
            alocal(i).wait()

        @pl.loop(0, NOS)
        def _(i):
            h2(i).wait_send()
            h3(i).wait_send()

    @pl.when(end)
    def _():
        for u in range(6):
            for j in range(1, 8):
                ag(u, j).wait_send()
        for c in metas(0, pbq):
            c.wait_send()

        @pl.loop(0, NAS)
        def _(i):
            a1(i).wait_send()
            a3(i).wait_recv()

        @pl.loop(0, NOS)
        def _(i):
            hlocal(i).wait()
            h1(i).wait_send()
            h3(i).wait_recv()


def _call(z_, h, lab, msk, gain, wT):
    T, D, V, RA, SG, PT, PV, OW = z_.T, z_.D, z_.V, z_.RA, z_.SG, z_.PT, z_.PV, z_.OW
    vm = pl.BlockSpec(memory_space=pltpu.VMEM)
    hb = pl.BlockSpec(memory_space=pl.ANY)
    outs = [jax.ShapeDtypeStruct(s, F32) for s in (
        (V, D), (T, D), (1, D), (8, 128), (4, V, PT), (3, T, D), (RA, D), (RA, D), (4, 4 * SG, D), (4, 2, SG, D), (4, 2, SG // 2, D))]
    bufs = [((T, D), BF16), ((T, D), BF16), ((RA + OW, D), F32), ((4, PV, PT), F32), ((3, PV, D), BF16), ((2, PT, D), F32), ((2, PT // 2, D), F32),
            ((max(z_.AG, SG), D), F32), ((SG // 2, D), BF16), ((2, 2, SG // 2, D), F32)]
    row = ((8, T),) * 3 + ((2, 8, T),) + tuple((int(k), 1, T) for k in "4233") + ((4, 2, T), (3, 2, T))
    tiles = ((2, 8, 128),) * 4 + ((6, 8, D), (5, 8, D))
    bufs += [(s, F32) for s in row + tiles]
    pairs = ((z_.NAS,),) * 6 + ((z_.NOS,),) * 6
    def shapes(text):
        return tuple(tuple(int(c) for c in w) for w in text.split("-"))

    sems = shapes("4-4-4-5-3") + pairs + ((z_.NOS,), (z_.NAS,)) + shapes("68-68-462-462-42-2-2-3-3-33-33-2-2-5-5")
    return pl.pallas_call(
        functools.partial(_kernel, z_),
        out_shape=outs,
        in_specs=[hb, vm, vm, vm, hb],
        out_specs=[hb, hb, vm, vm] + [hb] * (len(outs) - 4),
        scratch_shapes=[pltpu.VMEM(s, t) for s, t in bufs] + [pltpu.SemaphoreType.DMA(s) for s in sems],
        compiler_params=pltpu.CompilerParams(collective_id=0, has_side_effects=True, vmem_limit_bytes=1023 * 65536),
        name="lm_head",
    )(h, lab, msk, gain, wT)


def make(mesh, z_):
    def local_step(hidden, labels, loss_mask, norm_gain, w_shard):
        h = hidden.reshape(z_.T, z_.D)
        lab = labels.reshape(1, z_.T).astype(F32)
        msk = loss_mask.reshape(1, z_.T).astype(F32)
        gain = norm_gain.astype(F32).reshape(1, z_.D)
        o = _call(z_, h, lab, msk, gain, w_shard.T)
        dw, dh, dg, loss = o[:4]
        return loss[0, 0], dh.astype(BF16).reshape(hidden.shape), dg.reshape(z_.D), dw.T

    return jax.shard_map(local_step, mesh=mesh, in_specs=(P("dp", None, None), P("dp", None), P("dp", None), P(None), P(None, "tp")), out_specs=(P(), P("dp", None, None), P(None), P(None, "tp")), check_vma=False)


def solution(mesh):
    return make(mesh, Sizes(4096, 1024, 6288, 512, 2400, 480, 120, 496, 248, 256))
```

```python
import functools

import jax
import jax.numpy as jnp
from jax import lax
from jax.experimental import pallas as pl
from jax.experimental.pallas import tpu as pltpu
from jax.sharding import PartitionSpec as P

EPS_NORM = 1e-5
LOG2E = 1.4426950408889634
F32 = jnp.float32
BF16 = jnp.bfloat16
ANY = pl.ANY
NT = (((1,), (1,)), ((), ()))
TN = (((0,), (0,)), ((), ()))


class Sizes:
    def __init__(self, tokens, width, vocab, pv, own, oc, osub, ac, asub, st):
        self.T, self.D, self.V = tokens, width, vocab
        self.PV, self.ST = pv, st
        self.OW, self.OC, self.OS = own, oc, osub
        self.RA, self.AC, self.AS = vocab - 2 * own, ac, asub
        self.PT = tokens // 4
        self.SL = tokens // 8
        self.SK = self.SL // 2
        self.NPV = vocab // pv
        self.RV = vocab - self.NPV * pv
        self.SG = tokens // 32
        self.AG = (asub + 15) // 16 * 8
        self.NOS, self.NAS = own // osub, self.RA // asub


def _kernel(z_, h, lab, msk, gain, wT, dw, dh, dg, loss, zh, unf, rb, rc, dub0, dub1, dub2,
            uv, unv, pb, zr, wr, da, da2, stg, hst, dhs, m8, s8, t8, lab8, lsev, mnv, ltv, mskn, labn, sts, strv, cntb, cntr, lsb, lsr, dgb, dgr,
            zi, wi, zo, hs, lg, a1_s, a1_r, a2_s, a2_r, a3_s, a3_r, h1_s, h1_r, h2_s, h2_r, h3_s, h3_r, lo, la, ag_s, ag_r, du_s, du_r, dl, ct_s, ct_r, st_s, st_r, me_s, me_r, ls_s, ls_r, dg_s, dg_r):
    T, D, V = z_.T, z_.D, z_.V
    PV, ST, PT, SL, SK, NPV, RV, SG = z_.PV, z_.ST, z_.PT, z_.SL, z_.SK, z_.NPV, z_.RV, z_.SG
    OW, OC, OS, RA, AC, AS, AG, NOS, NAS = z_.OW, z_.OC, z_.OS, z_.RA, z_.AC, z_.AS, z_.AG, z_.NOS, z_.NAS
    NS = PT // ST
    d, t = lax.axis_index("dp"), lax.axis_index("tp")
    core, xx, yy = t % 2, (t // 2) % 2, t // 4
    tc, tx, ty = t + 1 - 2 * core, t + 2 - 4 * xx, t + 4 - 8 * yy
    da_, db_ = d + 1 - 2 * (d % 2), 3 - d
    df_ = 3 - da_
    mid = ((d + 1) // 2) % 2 == 1
    end = ((d + 1) // 2) % 2 == 0
    pc, px, py, pa, pbq, pf_ = (d, tc), (d, tx), (d, ty), (da_, t), (db_, t), (df_, t)
    own0 = (d // 3) * OW
    near0 = (da_ // 3) * OW
    far0 = OW - near0

    pair, quad = range(2), range(4)

    def al(x, m):
        return x if isinstance(x, int) else pl.multiple_of(x, m)

    def a8(x):
        return al(x, 8)

    def a16(x):
        return al(x, 16)

    def tof(x):
        return float(x) if isinstance(x, int) else x.astype(F32)

    def rcopy(src, dst, ssem, rsem, dev):
        return pltpu.make_async_remote_copy(src_ref=src, dst_ref=dst, send_sem=ssem, recv_sem=rsem, device_id=dev, device_id_type=pl.DeviceIdType.MESH)

    cp = pltpu.make_async_copy

    bar = pltpu.get_barrier_semaphore()
    for dev in (pc, px, py, pa, pbq, pf_):
        pl.semaphore_signal(bar, inc=1, device_id=dev, device_id_type=pl.DeviceIdType.MESH)
    hsl = cp(h.at[pl.ds(a16(t * SL), SL), :], wr.at[2, :SL, :], hs.at[4])
    hsl.start()

    def hcopy(b):
        return cp(h.at[pl.ds(a16(b * PT), PT), :], unv.at[pl.ds(a16(b * PT), PT), :], hs.at[b])

    for b in quad:
        hcopy(b).start()

    def wcopy(r0, n, slot):
        return cp(wT.at[pl.ds(r0, n), :], wr.at[slot, :n, :], wi.at[slot])

    wcopy(0, PV, 0).start()
    hsl.wait()

    def rms(hb):
        x = hb.astype(F32)
        inv = lax.rsqrt(jnp.mean(x * x, axis=1, keepdims=True) + EPS_NORM)
        return x * inv, inv

    xh, _ = rms(wr[2, :SL, :])
    ub0 = RA + OW - SL
    pb[ub0:ub0 + SL, :] = (xh * gain[...]).astype(BF16).astype(F32)
    sub_iota = lax.broadcasted_iota(jnp.int32, (8, T), 0).astype(F32)
    toff = (t * V).astype(F32)
    lab8[0] = jnp.broadcast_to(lab[...] - toff, (8, T)) - sub_iota
    cntb[0] = jnp.broadcast_to(jnp.sum(msk[...], axis=1, keepdims=True), (8, 128))
    m8[...] = jnp.full((8, T), -jnp.inf, F32)
    s8[...] = jnp.zeros((8, T), F32)
    t8[...] = jnp.zeros((8, T), F32)
    pl.semaphore_wait(bar, 6)

    def urow(tt, u):
        return unf.at[u // 2, pl.ds(a8(tt * SL + (u % 2) * SK), SK), :]

    def zsend(u, dev):
        return rcopy(pb.at[pl.ds(ub0 + (u % 2) * SK, SK), :], urow(t, u), ag_s.at[u, 0], ag_r.at[u, 0], dev)

    def metas(slot, dev):
        return [rcopy(src, dst.at[slot + o], me_s.at[i, slot], me_r.at[i, slot], dev)
                for i, (src, dst, o) in enumerate(((lab, labn, 0), (msk, mskn, 0), (lsev.at[0], lsev, 1)))]

    def ag(u, j):
        tf, tg = (tx, ty) if u % 2 == 0 else (ty, tx)
        pf, pg = (px, py) if u % 2 == 0 else (py, px)
        tfg = tf + tg - t
        who, dev = ((None, None), (t, pf), (t, pg), (tf, pg), (t, pc), (tf, pc), (tg, pc), (tfg, pc))[j]
        return rcopy(urow(who, u), urow(who, u), ag_s.at[u, j], ag_r.at[u, j], dev)

    def cnt2(i):
        return rcopy(cntb.at[i], cntr.at[i], ct_s.at[i], ct_r.at[i], (pa, pbq)[i])

    def lss2(i):
        return rcopy(lsb.at[i], lsr.at[i], ls_s.at[i], ls_r.at[i], (pa, pbq)[i])

    cnt2(0).start()

    @pl.when(mid)
    def _():
        for c in metas(1, pa)[:2] + metas(2, pf_)[:2]:
            c.start()

    @pl.when(end)
    def _():
        for c in metas(0, pbq)[:2]:
            c.start()
        for u in pair:
            zsend(u, pbq).start()

    def e1f(u):
        zsend(u, pa).wait_recv()
        ag(u, 1).start()

    def e1r(u):
        ag(u, 2).start()
        ag(u, 4).start()

    def e1(u):
        e1f(u)
        e1r(u)

    def e23(u):
        ag(u, 1).wait_recv()
        ag(u, 3).start()
        ag(u, 5).start()

    def e4(u):
        ag(u, 2).wait_recv()
        ag(u, 6).start()
        ag(u, 3).wait_recv()
        ag(u, 7).start()

    def ec(_):
        cnt2(0).wait()
        cntb[1] = cntb[0] + cntr[0]
        cnt2(1).start()

    def near(_):
        for u in range(2, 4):
            zsend(u, pa).start()

    def far(_):
        for u in range(4, 6):
            zsend(u, pf_).start()

    def run(evs, names):
        for i in range(0, len(evs), 2):
            names[evs[i]](int(evs[i + 1]))

    enames = dict(i=e1, j=e23, k=e4, m=e1f, n=e1r)
    early = dict(d="i0", g="i1", h="j0", k="m2")

    def stats(z, n, base, cols):
        labb = lab8[0, :, cols] - tof(base)
        m, s, tg = m8[:, cols], s8[:, cols], t8[:, cols]
        for w0 in range(0, n, 128):
            kk = min(128, n - w0)
            z3 = z[w0:w0 + kk].reshape(kk // 8, 8, ST)
            mn = jnp.maximum(m, jnp.max(z3, axis=0))
            mc = mn * LOG2E
            s = s * jnp.exp2(m * LOG2E - mc) + jnp.sum(jnp.exp2(z3 * LOG2E - mc[None]), axis=0)
            for i in range(kk // 8):
                tg = tg + jnp.where(labb == float(w0 + 8 * i), z3[i], 0.0)
            m = mn
        m8[:, cols], s8[:, cols], t8[:, cols] = m, s, tg

    def zout(tb, r0, n):
        return cp(zr.at[tb, :n, :], zh.at[tb, pl.ds(r0, n), :], zo.at[tb])

    def fwd_pieces(ws, tbs, r0, n):
        for tb in tbs:
            for k in range(NS):
                cols = pl.ds(al(tb * PT + k * ST, ST), ST)
                z = lax.dot_general(wr[ws, :n, :], uv[cols, :], NT, preferred_element_type=F32)
                zr[tb, :n, pl.ds(k * ST, ST)] = z
                stats(z, n, r0, cols)
            zout(tb, r0, n).start()

    @pl.loop(0, NPV)
    def _(v):
        r0 = a16(v * PV)
        ws = v % 2
        wcopy(r0, PV, ws).wait()

        @pl.when(v + 1 < NPV)
        def _():
            wcopy(a16(r0 + PV), PV, 1 - ws).start()

        for half in pair:
            tbs = (2 * half, 2 * half + 1)

            @pl.when(v == 0)
            def _():
                for tb in tbs:
                    hcopy(tb).wait()
                    rows = pl.ds(tb * PT, PT)
                    xb, _ = rms(unv[rows, :])
                    uv[rows, :] = (xb * gain[...]).astype(BF16)

            @pl.when(v > 0)
            def _():
                for tb in tbs:
                    zout(tb, 0, PV).wait()

            fwd_pieces(ws, tbs, r0, PV)

        def at(i):
            return v == min(i, NPV - 1)

        @pl.when(at(1))
        def _():
            ec(0)

        @pl.when(mid & at(5))
        def _():
            near(0)

        for ch, evs in early.items():
            @pl.when(end & at(ord(ch) - ord("a")))
            def _():
                run(evs, enames)

    wcopy(NPV * PV, RV, 2).start()
    wcopy(NPV * PV, RV, 2).wait()

    @pl.loop(0, 4)
    def _(tb):
        zout(tb, 0, PV).wait()
        fwd_pieces(2, (tb,), NPV * PV, RV)

    m = jnp.max(m8[...], axis=0, keepdims=True)
    s = jnp.sum(s8[...] * jnp.exp(m8[...] - m), axis=0, keepdims=True)
    sts[0, 0:1, :] = m + jnp.log(s)
    sts[0, 1:2, :] = jnp.sum(t8[...], axis=0, keepdims=True)
    for r, dev in enumerate((pc, px, py)):
        c = rcopy(sts.at[r], strv.at[r], st_s.at[r], st_r.at[r], dev)
        c.start()
        c.wait()
        a, b = sts[r, 0:1, :], strv[r, 0:1, :]
        hi = jnp.maximum(a, b)
        sts[r + 1, 0:1, :] = hi + jnp.log(jnp.exp(a - hi) + jnp.exp(b - hi))
        sts[r + 1, 1:2, :] = sts[r, 1:2, :] + strv[r, 1:2, :]
    lse, tgt = sts[3, 0:1, :], sts[3, 1:2, :]
    lsev[0] = lse * LOG2E
    cnt2(1).wait()
    cnt = (cntb[1] + cntr[1])[0:1, 0:1]
    mnv[0] = msk[...] / cnt
    ltv[0] = lsev[0] - jnp.log2(mnv[0])
    lsb[0] = jnp.broadcast_to(jnp.sum(msk[...] * (lse - tgt), axis=1, keepdims=True), (8, 128))

    @pl.when(mid)
    def _():
        metas(1, pa)[2].start()
        metas(2, pf_)[2].start()
        far(0)

    @pl.when(end)
    def _():
        metas(0, pbq)[2].start()
        run("n2j1k0", enames)

    lss2(0).start()
    for tb in quad:
        zout(tb, 0, RV).wait()

    def gmat(z, who, base, cols):
        one = 0 if who is None else 1
        labb = lab8[one, :, cols] - tof(base)
        mn = jnp.broadcast_to(mnv[one, :, cols], (8, ST))
        pm = jnp.exp2(z * LOG2E - ltv[one, :, cols])
        rows = []
        for i in range(z.shape[0] // 8):
            pi = pm[8 * i:8 * i + 8]
            rows.append(jnp.where(labb == float(8 * i), pi - mn, pi))
        return jnp.concatenate(rows, axis=0).astype(BF16)

    def arow(i):
        return pl.ds(a8(i * AS), AS)

    def awr(i):
        return dw.at[pl.ds(a8(2 * OW + i * AS), AS), :]

    def a1(i):
        return rcopy(pb.at[arow(i), :], rb.at[arow(i), :], a1_s.at[i], a1_r.at[i], pa)

    def a2(i):
        return rcopy(pb.at[arow(i), :], rc.at[arow(i), :], a2_s.at[i], a2_r.at[i], pbq)

    def a3(i):
        return rcopy(pb.at[arow(i), :], awr(i), a3_s.at[i], a3_r.at[i], pa)

    def alocal(i):
        return cp(pb.at[arow(i), :], awr(i), la.at[i])

    def grab(src, i):
        for o in range(0, AS, AG):
            n = min(AG, AS - o)
            rows = pl.ds(a8(i * AS + o), n)
            c = cp(src.at[rows, :], stg.at[:n, :], lg.at[0])
            c.start()
            c.wait()
            pb[rows, :] = pb[rows, :] + stg[:n, :]

    def ev_a1(i):
        a1(i).wait_recv()
        grab(rb, i)
        a2(i).start()

    def ev_a2(i):
        a2(i).wait()
        grab(rc, i)
        alocal(i).start()
        a3(i).start()

    def drow(base, i):
        return dw.at[pl.ds(a8(base + i * OS), OS), :]

    def prow(i):
        return pb.at[pl.ds(a8(RA + i * OS), OS), :]

    def h1(i):
        return rcopy(prow(i), drow(own0, i), h1_s.at[i], h1_r.at[i], pa)

    def h2(i):
        return rcopy(drow(near0, i), drow(near0, i), h2_s.at[i], h2_r.at[i], pbq)

    def h3(i):
        return rcopy(drow(far0, i), drow(far0, i), h3_s.at[i], h3_r.at[i], pa)

    def hop(i):
        h1(i).wait_recv()
        h2(i).start()
        if not isinstance(i, int) or i > 0:
            h2(i - 1).wait_recv()
            h3(i - 1).start()

    def hlocal(i):
        return cp(prow(i), drow(own0, i), lo.at[i])

    H = SG // 2
    k0 = core * (4 * SG)

    def lev(k):
        fb, sb = (xx, yy) if k == 0 else (yy, xx)
        pf, ps = (px, py) if k == 0 else (py, px)
        k1 = k * 2 * SG + fb * SG
        return pf, ps, k1, k * 2 * SG + (1 - fb) * SG, k1 + sb * H, k1 + (1 - sb) * H

    def ducopy(g, j, k=0):
        pf, ps, k1, o1, k2, o2 = lev(k)
        b = g % 2
        base = g * PT + k0
        sems = (du_s.at[g, j, k], du_r.at[g, j, k])
        if j == 0:
            return rcopy(da.at[b, pl.ds(a8(4 * SG - k0), 4 * SG), :], dub0.at[g], *sems, pc)
        if j == 1:
            return rcopy(da2.at[b, pl.ds(a8(o1), SG), :], dub1.at[g, k], *sems, pf)
        if j == 2:
            return rcopy(da2.at[b, pl.ds(a8(o2), H), :], dub2.at[g, k], *sems, ps)
        if j == 3:
            return rcopy(dhs.at[b, k], dh.at[pl.ds(a8(base + k2), H), :], *sems, ps)
        r, n, dev = ((k1, SG, pf), (0, 4 * SG, pc))[j - 4]
        r = dh.at[pl.ds(a8(base + r), n), :]
        return rcopy(r, r, *sems, dev)

    def add_in(buf, g, src, k, k2, n):
        @pl.loop(0, n // SG)
        def _(i):
            c = cp(buf.at[pl.ds(a8(i * SG), SG), :], stg.at[:SG, :], lg.at[1])
            c.start()
            c.wait()
            da2[g % 2, pl.ds(a8(k2 + i * SG), SG), :] = src[g % 2, pl.ds(a8(k + i * SG), SG), :] + stg[:SG, :]

    def d2(g):
        ducopy(g, 0).wait_recv()
        for k in pair:
            if g >= 2:
                ducopy(g - 2, 1, k).wait_send()
                ducopy(g - 2, 2, k).wait_send()
        add_in(dub0.at[g], g, da, k0, 0, 4 * SG)
        for k in pair:
            ducopy(g, 1, k).start()

    def d3(g):
        for k in pair:
            ducopy(g, 1, k).wait_recv()
            add_in(dub1.at[g, k], g, da2, lev(k)[2], lev(k)[2], SG)
            ducopy(g, 2, k).start()

    def dhlocal(g, k):
        return cp(dhs.at[g % 2, k], dh.at[pl.ds(a8(g * PT + k0 + lev(k)[4]), H), :], dl.at[g, k])

    def d4(g):
        for k in pair:
            k2 = lev(k)[4]
            ch = cp(h.at[pl.ds(a8(g * PT + k0 + k2), H), :], hst, lg.at[2])
            ch.start()
            ducopy(g, 2, k).wait_recv()
            c = cp(dub2.at[g, k], stg.at[:H, :], lg.at[1])
            c.start()
            c.wait()
            if g >= 2:
                ducopy(g - 2, 3, k).wait_send()
            ch.wait()
            xb, inv = rms(hst[...])
            du = da2[g % 2, pl.ds(a8(k2), H), :] + stg[:H, :]
            part = jnp.sum((du * xb).reshape(H // 8, 8, D), axis=0)
            dgb[0] = part if g == 0 and k == 0 else dgb[0] + part
            a = du * gain[...]
            dhs[g % 2, k] = inv * (a - xb * jnp.mean(a * xb, axis=1, keepdims=True))
            dhlocal(g, k).start()
            ducopy(g, 3, k).start()

    def d5(g):
        for k in pair:
            ducopy(g, 3, k).wait_recv()
            dhlocal(g, k).wait()
            ducopy(g, 4, k).start()

    def d6(g):
        for k in pair:
            ducopy(g, 4, k).wait_recv()
        ducopy(g, 5).start()

    dgdev = (pc, px, py, pa, pbq)

    def dgc(r):
        return rcopy(dgb.at[r], dgr.at[r], dg_s.at[r], dg_r.at[r], dgdev[r])

    def ev_dg(r):
        if r > 0:
            dgc(r - 1).wait()
            dgb[r] = dgb[r - 1] + dgr[r - 1]
        if r < 5:
            dgc(r).start()

    def ev_ls():
        lss2(0).wait()
        lsb[1] = lsb[0] + lsr[0]
        lss2(1).start()

    dnames = dict(a=d2, b=d3, c=d4, d=d5, e=d6, g=ev_dg)
    mnames = dict(p=ev_a1, q=ev_a2, h=hop)
    duev = dict(m1="a0", m2="b0a1", m3="c0a2", f3="b1")
    muev = dict(m1="p0", f1="p1", m2="q0p2", f2="q1", m3="p3q2")

    def poll(kind, idx):
        for i in quad:
            key = kind + str(i)
            if key in duev:
                @pl.when(idx == i)
                def _():
                    run(duev[key], dnames)
            if key in muev:
                @pl.when((idx == i) & mid)
                def _():
                    run(muev[key], mnames)

    def zin(tb, r0, n, slot):
        return cp(zh.at[tb, pl.ds(r0, n), :], zr.at[slot, :n, :], zi.at[slot])

    def uin(sh, b):
        n = PT // 2
        return cp(unf.at[sh, pl.ds(a8(b * n), n), :], zr.at[b % 4, :n, :], zi.at[b % 4])

    def convert(sh):
        for k in pair:
            for j in range(4, 8):
                ag_wait = rcopy(unf.at[0, :SK, :], unf.at[0, :SK, :], ag_s.at[2 * sh + k, j], ag_r.at[2 * sh + k, j], pc)
                ag_wait.wait_recv()
        for i, dst in enumerate((labn, mskn, lsev)):
            rcopy(dst.at[0], dst.at[0], me_s.at[i, sh], me_r.at[i, sh], pa).wait_recv()
        mnv[1] = mskn[sh] / cnt
        ltv[1] = lsev[sh + 1] - jnp.log2(mnv[1])
        lab8[1] = jnp.broadcast_to(labn[sh] - toff, (8, T)) - sub_iota
        for b in quad:
            uin(sh, b).start()

    def own_start(g0, n):
        for tb in quad:
            zin(tb, g0, n, tb).start()

    def chunk_own(r0, g0, n, more):
        rows = pl.ds(r0, n)
        pb[rows, :] = jnp.zeros((n, D), F32)

        @pl.loop(0, 4)
        def _(tb):
            zin(tb, g0, n, tb).wait()
            gs = []
            for k in range(NS):
                gs.append(gmat(zr[tb, :n, pl.ds(k * ST, ST)], None, g0, pl.ds(al(tb * PT + k * ST, ST), ST)))
            g = jnp.concatenate(gs, axis=1)

            @pl.when(more)
            def _():
                zin(tb, a8(g0 + n), n, tb).start()

            pb[rows, :] += jnp.dot(g, uv[pl.ds(a16(tb * PT), PT), :], preferred_element_type=F32)

    def chunk_far(r0, g0, n, sh, first):
        wcopy(g0, n, 0).start()
        wcopy(g0, n, 0).wait()
        rows = pl.ds(r0, n)

        @pl.loop(0, 2)
        def _(q):
            @pl.when(first)
            def _():
                for b in quad:
                    uin(sh, 4 * q + b).wait()
                    unv[pl.ds(a16((4 * q + b) * (PT // 2)), PT // 2), :] = zr[b, :PT // 2, :].astype(BF16)

                @pl.when(q == 0)
                def _():
                    for b in range(4, 8):
                        uin(sh, b).start()

            for j in pair:
                gs = []
                for k in range(NS):
                    cols = pl.ds(al((2 * q + j) * PT + k * ST, ST), ST)
                    z = lax.dot_general(wr[0, :n, :], unv[cols, :], NT, preferred_element_type=F32)
                    gs.append(gmat(z, sh, g0, cols))
                g = jnp.concatenate(gs, axis=1)
                pb[rows, :] += jnp.dot(g, unv[pl.ds(a16((2 * q + j) * PT), PT), :], preferred_element_type=F32)

    def du_piece(b, tb, v, r0, n):
        for k in range(NS):
            g = gmat(zr[v % 4, :n, pl.ds(k * ST, ST)], None, r0, pl.ds(al(tb * PT + k * ST, ST), ST))
            da[b, pl.ds(k * ST, ST), :] += lax.dot_general(g, wr[v % 3, :n, :], TN, preferred_element_type=F32)

    def du_block(tb):
        b = tb % 2

        def pz(v, n):
            return zin(tb, a16(v * PV), n, v % 4)

        def pw(v, n):
            return wcopy(a16(v * PV), n, v % 3)

        for g in range(2, 4):
            @pl.when(tb == g)
            def _():
                ducopy(g - 2, 0).wait_send()

        for v in pair:
            pz(v, PV).start()
            pw(v, PV).start()
        pz(2, PV).start()
        da[b] = jnp.zeros((PT, D), F32)

        @pl.loop(0, NPV)
        def _(v):
            pz(v, PV).wait()
            pw(v, PV).wait()
            for o, f in ((3, pz), (2, pw)):
                @pl.when(v + o < NPV)
                def _():
                    f(v + o, PV).start()

                @pl.when(v + o == NPV)
                def _():
                    f(NPV, RV).start()

            du_piece(b, tb, v, v * PV, PV)

            @pl.when(v == NPV // 2)
            def _():
                poll("m", tb)

        pz(NPV, RV).wait()
        pw(NPV, RV).wait()
        du_piece(b, tb, NPV, NPV * PV, RV)
        poll("f", tb)
        for g in quad:
            @pl.when(tb == g)
            def _():
                ducopy(g, 0).start()

    shev = dict(s00="j3i5", s02="j4k2", s04="k3", s11="j5", s14="k4k5")

    own_start(2 * OW, AC)

    @pl.loop(0, RA // AC)
    def _(c):
        chunk_own(a8(c * AC), a8(2 * OW + c * AC), AC, c + 1 < RA // AC)

        for i, evs in enumerate(("", "", "i3")):
            if evs:
                @pl.when(end & (c == i))
                def _():
                    run(evs, enames)

        @pl.when(end)
        def _():
            for s in range(AC // AS):
                a1(c * (AC // AS) + s).start()

    @pl.when(end)
    def _():
        own_start(a8(own0), OC)

        @pl.loop(0, OW // OC)
        def _(c):
            @pl.when(c == (ub0 - RA) // OC)
            def _():
                for u in pair:
                    zsend(u, pbq).wait_send()

            chunk_own(a8(RA + c * OC), a8(own0 + c * OC), OC, c + 1 < OW // OC)
            for i, evs in enumerate(("j2", "", "k1i4", "", "")):
                if evs:
                    @pl.when(c == i)
                    def _():
                        run(evs, enames)

        @pl.loop(0, 3)
        def _(sh):
            convert(sh)

            @pl.loop(0, OW // OC)
            def _(c):
                chunk_far(a8(RA + c * OC), a8(own0 + c * OC), OC, sh, c == 0)
                for x, evs in shev.items():
                    @pl.when((sh == int(x[1])) & (c == int(x[2])))
                    def _():
                        run(evs, enames)

                @pl.when(sh == 2)
                def _():
                    for s in range(OC // OS):
                        i = c * (OC // OS) + s
                        hlocal(i).start()
                        h1(i).start()

    @pl.loop(0, 4)
    def _(tb):
        du_block(tb)

    @pl.when(mid)
    def _():
        run("p4q3c1a3b2d0p5q4c2b3d1q5e0h0c3g0h1d2g1h2e1h3g2d3h4e2h5e3", {**dnames, **mnames})

        @pl.loop(6, NOS)
        def _(i):
            hop(i)

        h2(NOS - 1).wait_recv()
        h3(NOS - 1).start()

    @pl.when(end)
    def _():
        run("c1a3b2d0c2b3d1e0c3g0d2g1e1g2d3e2e3", dnames)

    run("g3g4", dnames)
    ev_ls()
    run("g5", dnames)

    dg[...] = jnp.sum(dgb[5], axis=0, keepdims=True)
    lss2(1).wait()
    loss[...] = (lsb[1] + lsr[1]) / cnt
    for g in quad:
        ducopy(g, 5).wait()
        for k in pair:
            ducopy(g, 4, k).wait_send()
            if g >= 2:
                for j in (1, 2, 3):
                    ducopy(g, j, k).wait_send()
        if g >= 2:
            ducopy(g, 0).wait_send()

    @pl.when(mid)
    def _():
        for u in range(2, 6):
            zsend(u, pa).wait_send()
        for c in metas(1, pa) + metas(2, pf_):
            c.wait_send()

        @pl.loop(0, NAS)
        def _(i):
            a3(i).wait_send()
            alocal(i).wait()

        @pl.loop(0, NOS)
        def _(i):
            h2(i).wait_send()
            h3(i).wait_send()

    @pl.when(end)
    def _():
        for u in range(6):
            for j in range(1, 8):
                ag(u, j).wait_send()
        for c in metas(0, pbq):
            c.wait_send()

        @pl.loop(0, NAS)
        def _(i):
            a1(i).wait_send()
            a3(i).wait_recv()

        @pl.loop(0, NOS)
        def _(i):
            hlocal(i).wait()
            h1(i).wait_send()
            h3(i).wait_recv()


def _call(z_, h, lab, msk, gain, wT):
    T, D, V, RA, SG, PT, PV, OW = z_.T, z_.D, z_.V, z_.RA, z_.SG, z_.PT, z_.PV, z_.OW
    vm = pl.BlockSpec(memory_space=pltpu.VMEM)
    hb = pl.BlockSpec(memory_space=pl.ANY)
    outs = [jax.ShapeDtypeStruct(s, F32) for s in (
        (V, D), (T, D), (1, D), (8, 128), (4, V, PT), (3, T, D), (RA, D), (RA, D), (4, 4 * SG, D), (4, 2, SG, D), (4, 2, SG // 2, D))]
    bufs = [((T, D), BF16), ((T, D), BF16), ((RA + OW, D), F32), ((4, PV, PT), F32), ((3, PV, D), BF16), ((2, PT, D), F32), ((2, PT // 2, D), F32),
            ((max(z_.AG, SG), D), F32), ((SG // 2, D), BF16), ((2, 2, SG // 2, D), F32)]
    row = ((8, T),) * 3 + ((2, 8, T),) + tuple((int(k), 1, T) for k in "42233") + ((4, 2, T), (3, 2, T))
    tiles = ((2, 8, 128),) * 4 + ((6, 8, D), (5, 8, D))
    bufs += [(s, F32) for s in row + tiles]
    pairs = ((z_.NAS,),) * 6 + ((z_.NOS,),) * 6
    def shapes(text):
        return tuple(tuple(int(c) for c in w) for w in text.split("-"))

    sems = shapes("4-4-4-5-3") + pairs + ((z_.NOS,), (z_.NAS,)) + shapes("68-68-462-462-42-2-2-3-3-33-33-2-2-5-5")
    return pl.pallas_call(
        functools.partial(_kernel, z_),
        out_shape=outs,
        in_specs=[hb, vm, vm, vm, hb],
        out_specs=[hb, hb, vm, vm] + [hb] * (len(outs) - 4),
        scratch_shapes=[pltpu.VMEM(s, t) for s, t in bufs] + [pltpu.SemaphoreType.DMA(s) for s in sems],
        compiler_params=pltpu.CompilerParams(collective_id=0, has_side_effects=True, vmem_limit_bytes=1023 * 65536),
        name="lm_head",
    )(h, lab, msk, gain, wT)


def make(mesh, z_):
    def local_step(hidden, labels, loss_mask, norm_gain, w_shard):
        h = hidden.reshape(z_.T, z_.D)
        lab = labels.reshape(1, z_.T).astype(F32)
        msk = loss_mask.reshape(1, z_.T).astype(F32)
        gain = norm_gain.astype(F32).reshape(1, z_.D)
        o = _call(z_, h, lab, msk, gain, w_shard.T)
        dw, dh, dg, loss = o[:4]
        return loss[0, 0], dh.astype(BF16).reshape(hidden.shape), dg.reshape(z_.D), dw.T

    return jax.shard_map(local_step, mesh=mesh, in_specs=(P("dp", None, None), P("dp", None), P("dp", None), P(None), P(None, "tp")), out_specs=(P(), P("dp", None, None), P(None), P(None, "tp")), check_vma=False)


def solution(mesh):
    return make(mesh, Sizes(4096, 1024, 6288, 512, 2400, 480, 120, 496, 248, 256))
```

```python
import functools

import jax
import jax.numpy as jnp
from jax import lax
from jax.experimental import pallas as pl
from jax.experimental.pallas import tpu as pltpu
from jax.sharding import PartitionSpec as P

EPS_NORM = 1e-5
LOG2E = 1.4426950408889634
F32 = jnp.float32
BF16 = jnp.bfloat16
ANY = pl.ANY
NT = (((1,), (1,)), ((), ()))
TN = (((0,), (0,)), ((), ()))


class Sizes:
    def __init__(self, tokens, width, vocab, pv, own, oc, osub, ac, asub, st):
        self.T, self.D, self.V = tokens, width, vocab
        self.PV, self.ST = pv, st
        self.OW, self.OC, self.OS = own, oc, osub
        self.RA, self.AC, self.AS = vocab - 2 * own, ac, asub
        self.PT = tokens // 4
        self.SL = tokens // 8
        self.SK = self.SL // 2
        self.NPV = vocab // pv
        self.RV = vocab - self.NPV * pv
        self.SG = tokens // 32
        self.AG = (asub + 15) // 16 * 8
        self.NOS, self.NAS = own // osub, self.RA // asub


def _kernel(z_, h, lab_, msk_, gain, wT, dw, dh, dg, loss, zh, unf, rb, rc, dub0, dub1, dub2,
            uv, unv, pb, zr, wr, da, da2, stg, hst, dhs, m8, s8, t8, lab, msk, lab8, lsev, mnv, ltv, mskn, labn, sts, strv, cntb, cntr, lsb, lsr, dgb, dgr,
            zi, wi, zo, hs, lg, a1_s, a1_r, a2_s, a2_r, a3_s, a3_r, h1_s, h1_r, h2_s, h2_r, h3_s, h3_r, lo, la, ag_s, ag_r, du_s, du_r, dl, ct_s, ct_r, st_s, st_r, me_s, me_r, ls_s, ls_r, dg_s, dg_r):
    T, D, V = z_.T, z_.D, z_.V
    PV, ST, PT, SL, SK, NPV, RV, SG = z_.PV, z_.ST, z_.PT, z_.SL, z_.SK, z_.NPV, z_.RV, z_.SG
    OW, OC, OS, RA, AC, AS, AG, NOS, NAS = z_.OW, z_.OC, z_.OS, z_.RA, z_.AC, z_.AS, z_.AG, z_.NOS, z_.NAS
    NS = PT // ST
    d, t = lax.axis_index("dp"), lax.axis_index("tp")
    core, xx, yy = t % 2, (t // 2) % 2, t // 4
    tc, tx, ty = t + 1 - 2 * core, t + 2 - 4 * xx, t + 4 - 8 * yy
    da_, db_ = d + 1 - 2 * (d % 2), 3 - d
    df_ = 3 - da_
    mid = ((d + 1) // 2) % 2 == 1
    end = ((d + 1) // 2) % 2 == 0
    pc, px, py, pa, pbq, pf_ = (d, tc), (d, tx), (d, ty), (da_, t), (db_, t), (df_, t)
    own0 = (d // 3) * OW
    near0 = (da_ // 3) * OW
    far0 = OW - near0

    pair, quad = range(2), range(4)

    def al(x, m):
        return x if isinstance(x, int) else pl.multiple_of(x, m)

    def a8(x):
        return al(x, 8)

    def a16(x):
        return al(x, 16)

    def tof(x):
        return float(x) if isinstance(x, int) else x.astype(F32)

    def rcopy(src, dst, ssem, rsem, dev):
        return pltpu.make_async_remote_copy(src_ref=src, dst_ref=dst, send_sem=ssem, recv_sem=rsem, device_id=dev, device_id_type=pl.DeviceIdType.MESH)

    cp = pltpu.make_async_copy

    bar = pltpu.get_barrier_semaphore()
    for dev in (pc, px, py, pa, pbq, pf_):
        pl.semaphore_signal(bar, inc=1, device_id=dev, device_id_type=pl.DeviceIdType.MESH)
    hsl = cp(h.at[pl.ds(a16(t * SL), SL), :], wr.at[2, :SL, :], hs.at[4])
    hsl.start()

    def hcopy(b):
        return cp(h.at[pl.ds(a16(b * PT), PT), :], unv.at[pl.ds(a16(b * PT), PT), :], hs.at[b])

    for b in quad:
        hcopy(b).start()

    def wcopy(r0, n, slot):
        return cp(wT.at[pl.ds(r0, n), :], wr.at[slot, :n, :], wi.at[slot])

    wcopy(0, PV, 0).start()
    hsl.wait()

    def rms(hb):
        x = hb.astype(F32)
        inv = lax.rsqrt(jnp.mean(x * x, axis=1, keepdims=True) + EPS_NORM)
        return x * inv, inv

    n = lab_.shape[1]
    for b in range(T // n):
        lab[:, pl.ds(b * n, n)] = lab_[pl.ds(b, 1), :].astype(F32)
        msk[:, pl.ds(b * n, n)] = msk_[pl.ds(b, 1), :].astype(F32)
    xh, _ = rms(wr[2, :SL, :])
    ub0 = RA + OW - SL
    pb[ub0:ub0 + SL, :] = (xh * gain[...]).astype(BF16).astype(F32)
    sub_iota = lax.broadcasted_iota(jnp.int32, (8, T), 0).astype(F32)
    toff = (t * V).astype(F32)
    lab8[0] = jnp.broadcast_to(lab[...] - toff, (8, T)) - sub_iota
    cntb[0] = jnp.broadcast_to(jnp.sum(msk[...], axis=1, keepdims=True), (8, 128))
    m8[...] = jnp.full((8, T), -jnp.inf, F32)
    s8[...] = jnp.zeros((8, T), F32)
    t8[...] = jnp.zeros((8, T), F32)
    pl.semaphore_wait(bar, 6)

    def urow(tt, u):
        return unf.at[u // 2, pl.ds(a8(tt * SL + (u % 2) * SK), SK), :]

    def zsend(u, dev):
        return rcopy(pb.at[pl.ds(ub0 + (u % 2) * SK, SK), :], urow(t, u), ag_s.at[u, 0], ag_r.at[u, 0], dev)

    def metas(slot, dev):
        return [rcopy(src, dst.at[slot + o], me_s.at[i, slot], me_r.at[i, slot], dev)
                for i, (src, dst, o) in enumerate(((lab, labn, 0), (msk, mskn, 0), (lsev.at[0], lsev, 1)))]

    def ag(u, j):
        tf, tg = (tx, ty) if u % 2 == 0 else (ty, tx)
        pf, pg = (px, py) if u % 2 == 0 else (py, px)
        tfg = tf + tg - t
        who, dev = ((None, None), (t, pf), (t, pg), (tf, pg), (t, pc), (tf, pc), (tg, pc), (tfg, pc))[j]
        return rcopy(urow(who, u), urow(who, u), ag_s.at[u, j], ag_r.at[u, j], dev)

    def cnt2(i):
        return rcopy(cntb.at[i], cntr.at[i], ct_s.at[i], ct_r.at[i], (pa, pbq)[i])

    def lss2(i):
        return rcopy(lsb.at[i], lsr.at[i], ls_s.at[i], ls_r.at[i], (pa, pbq)[i])

    cnt2(0).start()

    @pl.when(mid)
    def _():
        for c in metas(1, pa)[:2] + metas(2, pf_)[:2]:
            c.start()

    @pl.when(end)
    def _():
        for c in metas(0, pbq)[:2]:
            c.start()
        for u in pair:
            zsend(u, pbq).start()

    def e1f(u):
        zsend(u, pa).wait_recv()
        ag(u, 1).start()

    def e1r(u):
        ag(u, 2).start()
        ag(u, 4).start()

    def e1(u):
        e1f(u)
        e1r(u)

    def e23(u):
        ag(u, 1).wait_recv()
        ag(u, 3).start()
        ag(u, 5).start()

    def e4(u):
        ag(u, 2).wait_recv()
        ag(u, 6).start()
        ag(u, 3).wait_recv()
        ag(u, 7).start()

    def ec(_):
        cnt2(0).wait()
        cntb[1] = cntb[0] + cntr[0]
        cnt2(1).start()

    def near(_):
        for u in range(2, 4):
            zsend(u, pa).start()

    def far(_):
        for u in range(4, 6):
            zsend(u, pf_).start()

    def run(evs, names):
        for i in range(0, len(evs), 2):
            names[evs[i]](int(evs[i + 1]))

    enames = dict(i=e1, j=e23, k=e4, m=e1f, n=e1r)
    early = dict(d="i0", g="i1", h="j0", k="m2")

    def stats(z, n, base, cols):
        labb = lab8[0, :, cols] - tof(base)
        m, s, tg = m8[:, cols], s8[:, cols], t8[:, cols]
        for w0 in range(0, n, 128):
            kk = min(128, n - w0)
            z3 = z[w0:w0 + kk].reshape(kk // 8, 8, ST)
            mn = jnp.maximum(m, jnp.max(z3, axis=0))
            mc = mn * LOG2E
            s = s * jnp.exp2(m * LOG2E - mc) + jnp.sum(jnp.exp2(z3 * LOG2E - mc[None]), axis=0)
            for i in range(kk // 8):
                tg = tg + jnp.where(labb == float(w0 + 8 * i), z3[i], 0.0)
            m = mn
        m8[:, cols], s8[:, cols], t8[:, cols] = m, s, tg

    def zout(tb, r0, n):
        return cp(zr.at[tb, :n, :], zh.at[tb, pl.ds(r0, n), :], zo.at[tb])

    def fwd_pieces(ws, tbs, r0, n):
        for tb in tbs:
            for k in range(NS):
                cols = pl.ds(al(tb * PT + k * ST, ST), ST)
                z = lax.dot_general(wr[ws, :n, :], uv[cols, :], NT, preferred_element_type=F32)
                zr[tb, :n, pl.ds(k * ST, ST)] = z
                stats(z, n, r0, cols)
            zout(tb, r0, n).start()

    @pl.loop(0, NPV)
    def _(v):
        r0 = a16(v * PV)
        ws = v % 2
        wcopy(r0, PV, ws).wait()

        @pl.when(v + 1 < NPV)
        def _():
            wcopy(a16(r0 + PV), PV, 1 - ws).start()

        for half in pair:
            tbs = (2 * half, 2 * half + 1)

            @pl.when(v == 0)
            def _():
                for tb in tbs:
                    hcopy(tb).wait()
                    rows = pl.ds(tb * PT, PT)
                    xb, _ = rms(unv[rows, :])
                    uv[rows, :] = (xb * gain[...]).astype(BF16)

            @pl.when(v > 0)
            def _():
                for tb in tbs:
                    zout(tb, 0, PV).wait()

            fwd_pieces(ws, tbs, r0, PV)

        def at(i):
            return v == min(i, NPV - 1)

        @pl.when(at(1))
        def _():
            ec(0)

        @pl.when(mid & at(5))
        def _():
            near(0)

        for ch, evs in early.items():
            @pl.when(end & at(ord(ch) - ord("a")))
            def _():
                run(evs, enames)

    wcopy(NPV * PV, RV, 2).start()
    wcopy(NPV * PV, RV, 2).wait()

    @pl.loop(0, 4)
    def _(tb):
        zout(tb, 0, PV).wait()
        fwd_pieces(2, (tb,), NPV * PV, RV)

    m = jnp.max(m8[...], axis=0, keepdims=True)
    s = jnp.sum(s8[...] * jnp.exp(m8[...] - m), axis=0, keepdims=True)
    sts[0, 0:1, :] = m + jnp.log(s)
    sts[0, 1:2, :] = jnp.sum(t8[...], axis=0, keepdims=True)
    for r, dev in enumerate((pc, px, py)):
        c = rcopy(sts.at[r], strv.at[r], st_s.at[r], st_r.at[r], dev)
        c.start()
        c.wait()
        a, b = sts[r, 0:1, :], strv[r, 0:1, :]
        hi = jnp.maximum(a, b)
        sts[r + 1, 0:1, :] = hi + jnp.log(jnp.exp(a - hi) + jnp.exp(b - hi))
        sts[r + 1, 1:2, :] = sts[r, 1:2, :] + strv[r, 1:2, :]
    lse, tgt = sts[3, 0:1, :], sts[3, 1:2, :]
    lsev[0] = lse * LOG2E
    cnt2(1).wait()
    cnt = (cntb[1] + cntr[1])[0:1, 0:1]
    mnv[0] = msk[...] / cnt
    ltv[0] = lsev[0] - jnp.log2(mnv[0])
    lsb[0] = jnp.broadcast_to(jnp.sum(msk[...] * (lse - tgt), axis=1, keepdims=True), (8, 128))

    @pl.when(mid)
    def _():
        metas(1, pa)[2].start()
        metas(2, pf_)[2].start()
        far(0)

    @pl.when(end)
    def _():
        metas(0, pbq)[2].start()
        run("n2j1k0", enames)

    lss2(0).start()
    for tb in quad:
        zout(tb, 0, RV).wait()

    def gmat(z, who, base, cols):
        one = 0 if who is None else 1
        labb = lab8[one, :, cols] - tof(base)
        mn = jnp.broadcast_to(mnv[one, :, cols], (8, ST))
        pm = jnp.exp2(z * LOG2E - ltv[one, :, cols])
        rows = []
        for i in range(z.shape[0] // 8):
            pi = pm[8 * i:8 * i + 8]
            rows.append(jnp.where(labb == float(8 * i), pi - mn, pi))
        return jnp.concatenate(rows, axis=0).astype(BF16)

    def arow(i):
        return pl.ds(a8(i * AS), AS)

    def awr(i):
        return dw.at[pl.ds(a8(2 * OW + i * AS), AS), :]

    def a1(i):
        return rcopy(pb.at[arow(i), :], rb.at[arow(i), :], a1_s.at[i], a1_r.at[i], pa)

    def a2(i):
        return rcopy(pb.at[arow(i), :], rc.at[arow(i), :], a2_s.at[i], a2_r.at[i], pbq)

    def a3(i):
        return rcopy(pb.at[arow(i), :], awr(i), a3_s.at[i], a3_r.at[i], pa)

    def alocal(i):
        return cp(pb.at[arow(i), :], awr(i), la.at[i])

    def grab(src, i):
        for o in range(0, AS, AG):
            n = min(AG, AS - o)
            rows = pl.ds(a8(i * AS + o), n)
            c = cp(src.at[rows, :], stg.at[:n, :], lg.at[0])
            c.start()
            c.wait()
            pb[rows, :] = pb[rows, :] + stg[:n, :]

    def ev_a1(i):
        a1(i).wait_recv()
        grab(rb, i)
        a2(i).start()

    def ev_a2(i):
        a2(i).wait()
        grab(rc, i)
        alocal(i).start()
        a3(i).start()

    def drow(base, i):
        return dw.at[pl.ds(a8(base + i * OS), OS), :]

    def prow(i):
        return pb.at[pl.ds(a8(RA + i * OS), OS), :]

    def h1(i):
        return rcopy(prow(i), drow(own0, i), h1_s.at[i], h1_r.at[i], pa)

    def h2(i):
        return rcopy(drow(near0, i), drow(near0, i), h2_s.at[i], h2_r.at[i], pbq)

    def h3(i):
        return rcopy(drow(far0, i), drow(far0, i), h3_s.at[i], h3_r.at[i], pa)

    def hop(i):
        h1(i).wait_recv()
        h2(i).start()
        if not isinstance(i, int) or i > 0:
            h2(i - 1).wait_recv()
            h3(i - 1).start()

    def hlocal(i):
        return cp(prow(i), drow(own0, i), lo.at[i])

    H = SG // 2
    k0 = core * (4 * SG)

    def lev(k):
        fb, sb = (xx, yy) if k == 0 else (yy, xx)
        pf, ps = (px, py) if k == 0 else (py, px)
        k1 = k * 2 * SG + fb * SG
        return pf, ps, k1, k * 2 * SG + (1 - fb) * SG, k1 + sb * H, k1 + (1 - sb) * H

    def ducopy(g, j, k=0):
        pf, ps, k1, o1, k2, o2 = lev(k)
        b = g % 2
        base = g * PT + k0
        sems = (du_s.at[g, j, k], du_r.at[g, j, k])
        if j == 0:
            return rcopy(da.at[b, pl.ds(a8(4 * SG - k0), 4 * SG), :], dub0.at[g], *sems, pc)
        if j == 1:
            return rcopy(da2.at[b, pl.ds(a8(o1), SG), :], dub1.at[g, k], *sems, pf)
        if j == 2:
            return rcopy(da2.at[b, pl.ds(a8(o2), H), :], dub2.at[g, k], *sems, ps)
        if j == 3:
            return rcopy(dhs.at[b, k], dh.at[pl.ds(a8(base + k2), H), :], *sems, ps)
        r, n, dev = ((k1, SG, pf), (0, 4 * SG, pc))[j - 4]
        r = dh.at[pl.ds(a8(base + r), n), :]
        return rcopy(r, r, *sems, dev)

    def add_in(buf, g, src, k, k2, n):
        @pl.loop(0, n // SG)
        def _(i):
            c = cp(buf.at[pl.ds(a8(i * SG), SG), :], stg.at[:SG, :], lg.at[1])
            c.start()
            c.wait()
            da2[g % 2, pl.ds(a8(k2 + i * SG), SG), :] = src[g % 2, pl.ds(a8(k + i * SG), SG), :] + stg[:SG, :]

    def d2(g):
        ducopy(g, 0).wait_recv()
        for k in pair:
            if g >= 2:
                ducopy(g - 2, 1, k).wait_send()
                ducopy(g - 2, 2, k).wait_send()
        add_in(dub0.at[g], g, da, k0, 0, 4 * SG)
        for k in pair:
            ducopy(g, 1, k).start()

    def d3(g):
        for k in pair:
            ducopy(g, 1, k).wait_recv()
            add_in(dub1.at[g, k], g, da2, lev(k)[2], lev(k)[2], SG)
            ducopy(g, 2, k).start()

    def dhlocal(g, k):
        return cp(dhs.at[g % 2, k], dh.at[pl.ds(a8(g * PT + k0 + lev(k)[4]), H), :], dl.at[g, k])

    def d4(g):
        for k in pair:
            k2 = lev(k)[4]
            ch = cp(h.at[pl.ds(a8(g * PT + k0 + k2), H), :], hst, lg.at[2])
            ch.start()
            ducopy(g, 2, k).wait_recv()
            c = cp(dub2.at[g, k], stg.at[:H, :], lg.at[1])
            c.start()
            c.wait()
            if g >= 2:
                ducopy(g - 2, 3, k).wait_send()
            ch.wait()
            xb, inv = rms(hst[...])
            du = da2[g % 2, pl.ds(a8(k2), H), :] + stg[:H, :]
            part = jnp.sum((du * xb).reshape(H // 8, 8, D), axis=0)
            dgb[0] = part if g == 0 and k == 0 else dgb[0] + part
            a = du * gain[...]
            dhs[g % 2, k] = inv * (a - xb * jnp.mean(a * xb, axis=1, keepdims=True))
            dhlocal(g, k).start()
            ducopy(g, 3, k).start()

    def d5(g):
        for k in pair:
            ducopy(g, 3, k).wait_recv()
            dhlocal(g, k).wait()
            ducopy(g, 4, k).start()

    def d6(g):
        for k in pair:
            ducopy(g, 4, k).wait_recv()
        ducopy(g, 5).start()

    dgdev = (pc, px, py, pa, pbq)

    def dgc(r):
        return rcopy(dgb.at[r], dgr.at[r], dg_s.at[r], dg_r.at[r], dgdev[r])

    def ev_dg(r):
        if r > 0:
            dgc(r - 1).wait()
            dgb[r] = dgb[r - 1] + dgr[r - 1]
        if r < 5:
            dgc(r).start()

    def ev_ls():
        lss2(0).wait()
        lsb[1] = lsb[0] + lsr[0]
        lss2(1).start()

    dnames = dict(a=d2, b=d3, c=d4, d=d5, e=d6, g=ev_dg)
    mnames = dict(p=ev_a1, q=ev_a2, h=hop)
    duev = dict(m1="a0", m2="b0a1", m3="c0a2", f3="b1d0")
    muev = dict(m1="p0", f1="p1", m2="q0p2", f2="q1", m3="p3q2")

    def poll(kind, idx):
        for i in quad:
            key = kind + str(i)
            if key in duev:
                @pl.when(idx == i)
                def _():
                    run(duev[key], dnames)
            if key in muev:
                @pl.when((idx == i) & mid)
                def _():
                    run(muev[key], mnames)

    def zin(tb, r0, n, slot):
        return cp(zh.at[tb, pl.ds(r0, n), :], zr.at[slot, :n, :], zi.at[slot])

    def uin(sh, b):
        n = PT // 2
        return cp(unf.at[sh, pl.ds(a8(b * n), n), :], zr.at[b % 4, :n, :], zi.at[b % 4])

    def convert(sh):
        for k in pair:
            for j in range(4, 8):
                ag_wait = rcopy(unf.at[0, :SK, :], unf.at[0, :SK, :], ag_s.at[2 * sh + k, j], ag_r.at[2 * sh + k, j], pc)
                ag_wait.wait_recv()
        for i, dst in enumerate((labn, mskn, lsev)):
            rcopy(dst.at[0], dst.at[0], me_s.at[i, sh], me_r.at[i, sh], pa).wait_recv()
        mnv[1] = mskn[sh] / cnt
        ltv[1] = lsev[sh + 1] - jnp.log2(mnv[1])
        lab8[1] = jnp.broadcast_to(labn[sh] - toff, (8, T)) - sub_iota
        for b in quad:
            uin(sh, b).start()

    def own_start(g0, n):
        for tb in quad:
            zin(tb, g0, n, tb).start()

    def chunk_own(r0, g0, n, more):
        rows = pl.ds(r0, n)
        pb[rows, :] = jnp.zeros((n, D), F32)

        @pl.loop(0, 4)
        def _(tb):
            zin(tb, g0, n, tb).wait()
            gs = []
            for k in range(NS):
                gs.append(gmat(zr[tb, :n, pl.ds(k * ST, ST)], None, g0, pl.ds(al(tb * PT + k * ST, ST), ST)))
            g = jnp.concatenate(gs, axis=1)

            @pl.when(more)
            def _():
                zin(tb, a8(g0 + n), n, tb).start()

            pb[rows, :] += jnp.dot(g, uv[pl.ds(a16(tb * PT), PT), :], preferred_element_type=F32)

    def chunk_far(r0, g0, n, sh, first):
        wcopy(g0, n, 0).start()
        wcopy(g0, n, 0).wait()
        rows = pl.ds(r0, n)

        @pl.loop(0, 2)
        def _(q):
            @pl.when(first)
            def _():
                for b in quad:
                    uin(sh, 4 * q + b).wait()
                    unv[pl.ds(a16((4 * q + b) * (PT // 2)), PT // 2), :] = zr[b, :PT // 2, :].astype(BF16)

                @pl.when(q == 0)
                def _():
                    for b in range(4, 8):
                        uin(sh, b).start()

            for j in pair:
                gs = []
                for k in range(NS):
                    cols = pl.ds(al((2 * q + j) * PT + k * ST, ST), ST)
                    z = lax.dot_general(wr[0, :n, :], unv[cols, :], NT, preferred_element_type=F32)
                    gs.append(gmat(z, sh, g0, cols))
                g = jnp.concatenate(gs, axis=1)
                pb[rows, :] += jnp.dot(g, unv[pl.ds(a16((2 * q + j) * PT), PT), :], preferred_element_type=F32)

    def du_piece(b, tb, v, r0, n):
        for k in range(NS):
            g = gmat(zr[v % 4, :n, pl.ds(k * ST, ST)], None, r0, pl.ds(al(tb * PT + k * ST, ST), ST))
            da[b, pl.ds(k * ST, ST), :] += lax.dot_general(g, wr[v % 3, :n, :], TN, preferred_element_type=F32)

    def du_block(tb):
        b = tb % 2

        def pz(v, n):
            return zin(tb, a16(v * PV), n, v % 4)

        def pw(v, n):
            return wcopy(a16(v * PV), n, v % 3)

        for g in range(2, 4):
            @pl.when(tb == g)
            def _():
                ducopy(g - 2, 0).wait_send()

        for v in pair:
            pz(v, PV).start()
            pw(v, PV).start()
        pz(2, PV).start()
        da[b] = jnp.zeros((PT, D), F32)

        @pl.loop(0, NPV)
        def _(v):
            pz(v, PV).wait()
            pw(v, PV).wait()
            for o, f in ((3, pz), (2, pw)):
                @pl.when(v + o < NPV)
                def _():
                    f(v + o, PV).start()

                @pl.when(v + o == NPV)
                def _():
                    f(NPV, RV).start()

            du_piece(b, tb, v, v * PV, PV)

            @pl.when(v == NPV // 2)
            def _():
                poll("m", tb)

        pz(NPV, RV).wait()
        pw(NPV, RV).wait()
        du_piece(b, tb, NPV, NPV * PV, RV)
        poll("f", tb)
        for g in quad:
            @pl.when(tb == g)
            def _():
                ducopy(g, 0).start()

    shev = dict(s00="j3i5", s02="j4k2", s04="k3", s11="j5", s14="k4k5")

    own_start(2 * OW, AC)

    @pl.loop(0, RA // AC)
    def _(c):
        chunk_own(a8(c * AC), a8(2 * OW + c * AC), AC, c + 1 < RA // AC)

        for i, evs in enumerate(("", "", "i3")):
            if evs:
                @pl.when(end & (c == i))
                def _():
                    run(evs, enames)

        @pl.when(end)
        def _():
            for s in range(AC // AS):
                a1(c * (AC // AS) + s).start()

    @pl.when(end)
    def _():
        own_start(a8(own0), OC)

        @pl.loop(0, OW // OC)
        def _(c):
            @pl.when(c == (ub0 - RA) // OC)
            def _():
                for u in pair:
                    zsend(u, pbq).wait_send()

            chunk_own(a8(RA + c * OC), a8(own0 + c * OC), OC, c + 1 < OW // OC)
            for i, evs in enumerate(("j2", "", "k1i4", "", "")):
                if evs:
                    @pl.when(c == i)
                    def _():
                        run(evs, enames)

        @pl.loop(0, 3)
        def _(sh):
            convert(sh)

            @pl.loop(0, OW // OC)
            def _(c):
                chunk_far(a8(RA + c * OC), a8(own0 + c * OC), OC, sh, c == 0)
                for x, evs in shev.items():
                    @pl.when((sh == int(x[1])) & (c == int(x[2])))
                    def _():
                        run(evs, enames)

                @pl.when(sh == 2)
                def _():
                    for s in range(OC // OS):
                        i = c * (OC // OS) + s
                        hlocal(i).start()
                        h1(i).start()

    @pl.loop(0, 4)
    def _(tb):
        du_block(tb)

    @pl.when(mid)
    def _():
        run("p4q3c1a3b2p5q4c2b3d1q5e0h0c3g0h1d2g1h2e1h3g2d3h4g3e2h5e3", {**dnames, **mnames})

        @pl.loop(6, NOS)
        def _(i):
            hop(i)

        h2(NOS - 1).wait_recv()
        h3(NOS - 1).start()

    @pl.when(end)
    def _():
        run("c1a3b2b3c2d1e0c3g0d2d3e1g1e2g2e3g3", dnames)

    run("g4", dnames)
    ev_ls()
    run("g5", dnames)

    dg[...] = jnp.sum(dgb[5], axis=0, keepdims=True)
    lss2(1).wait()
    loss[...] = (lsb[1] + lsr[1]) / cnt
    for g in quad:
        ducopy(g, 5).wait()
        for k in pair:
            ducopy(g, 4, k).wait_send()
            if g >= 2:
                for j in (1, 2, 3):
                    ducopy(g, j, k).wait_send()
        if g >= 2:
            ducopy(g, 0).wait_send()

    @pl.when(mid)
    def _():
        for u in range(2, 6):
            zsend(u, pa).wait_send()
        for c in metas(1, pa) + metas(2, pf_):
            c.wait_send()

        @pl.loop(0, NAS)
        def _(i):
            a3(i).wait_send()
            alocal(i).wait()

        @pl.loop(0, NOS)
        def _(i):
            h2(i).wait_send()
            h3(i).wait_send()

    @pl.when(end)
    def _():
        for u in range(6):
            for j in range(1, 8):
                ag(u, j).wait_send()
        for c in metas(0, pbq):
            c.wait_send()

        @pl.loop(0, NAS)
        def _(i):
            a1(i).wait_send()
            a3(i).wait_recv()

        @pl.loop(0, NOS)
        def _(i):
            hlocal(i).wait()
            h1(i).wait_send()
            h3(i).wait_recv()


def _call(z_, h, lab, msk, gain, wT):
    T, D, V, RA, SG, PT, PV, OW = z_.T, z_.D, z_.V, z_.RA, z_.SG, z_.PT, z_.PV, z_.OW
    vm = pl.BlockSpec(memory_space=pltpu.VMEM)
    hb = pl.BlockSpec(memory_space=pl.ANY)
    outs = [jax.ShapeDtypeStruct(s, F32) for s in (
        (V, D), (T, D), (1, D), (8, 128), (4, V, PT), (3, T, D), (RA, D), (RA, D), (4, 4 * SG, D), (4, 2, SG, D), (4, 2, SG // 2, D))]
    bufs = [((T, D), BF16), ((T, D), BF16), ((RA + OW, D), F32), ((4, PV, PT), F32), ((3, PV, D), BF16), ((2, PT, D), F32), ((2, PT // 2, D), F32),
            ((max(z_.AG, SG), D), F32), ((SG // 2, D), BF16), ((2, 2, SG // 2, D), F32)]
    row = ((8, T),) * 3 + ((1, T),) * 2 + ((2, 8, T),) + tuple((int(k), 1, T) for k in "42233") + ((4, 2, T), (3, 2, T))
    tiles = ((2, 8, 128),) * 4 + ((6, 8, D), (5, 8, D))
    bufs += [(s, F32) for s in row + tiles]
    pairs = ((z_.NAS,),) * 6 + ((z_.NOS,),) * 6
    def shapes(text):
        return tuple(tuple(int(c) for c in w) for w in text.split("-"))

    sems = shapes("4-4-4-5-3") + pairs + ((z_.NOS,), (z_.NAS,)) + shapes("68-68-462-462-42-2-2-3-3-33-33-2-2-5-5")
    return pl.pallas_call(
        functools.partial(_kernel, z_),
        out_shape=outs,
        in_specs=[hb, vm, vm, vm, hb],
        out_specs=[hb, hb, vm, vm] + [hb] * (len(outs) - 4),
        scratch_shapes=[pltpu.VMEM(s, t) for s, t in bufs] + [pltpu.SemaphoreType.DMA(s) for s in sems],
        compiler_params=pltpu.CompilerParams(collective_id=0, has_side_effects=True, vmem_limit_bytes=1023 * 65536),
        name="lm_head",
    )(h, lab, msk, gain, wT)


def make(mesh, z_):
    def local_step(hidden, labels, loss_mask, norm_gain, w_shard):
        h = hidden.reshape(z_.T, z_.D)
        gain = norm_gain.astype(F32).reshape(1, z_.D)
        o = _call(z_, h, labels, loss_mask, gain, w_shard.T)
        dw, dh, dg, loss = o[:4]
        return loss[0, 0], dh.astype(BF16).reshape(hidden.shape), dg.reshape(z_.D), dw.T

    return jax.shard_map(local_step, mesh=mesh, in_specs=(P("dp", None, None), P("dp", None), P("dp", None), P(None), P(None, "tp")), out_specs=(P(), P("dp", None, None), P(None), P(None, "tp")), check_vma=False)


def solution(mesh):
    return make(mesh, Sizes(4096, 1024, 6288, 512, 2400, 480, 120, 496, 248, 256))
```
